32 devices in a mesh: rows: 8 (over z, x), ka: 4 (over y, core).
Axes of the slice: x: 2, y: 2, z: 4, core: 2. Of those that a mesh axis runs over, the one named last changes fastest.
Arguments:
- pair_repr: bfloat16 [512, 512, 128], P('rows', 'ka'), may hold values from -6 to 6
- pair_mask: int32 [512, 512], P('rows', 'ka'), may hold values 0 or 1
- ln_gain: float32 [128], replicated, may hold values from 0.1 to 1.9
- ln_bias: float32 [128], replicated, may hold values from -3 to 3
- w_proj: bfloat16 [128, 256], replicated, may hold values from -0.5 to 0.5
- w_gate: bfloat16 [128, 256], replicated, may hold values from -0.5 to 0.5
- w_out_gate: bfloat16 [128, 128], replicated, may hold values from -0.5 to 0.5
- out_gain: float32 [128], replicated, may hold values from 0.1 to 1.9
- out_bias: float32 [128], replicated, may hold values from -3 to 3
- w_out: bfloat16 [128, 128], replicated, may hold values from -0.5 to 0.5
Outputs:
- update: bfloat16 [512, 512, 128], P('rows', 'ka')
The draws below stay inside these ranges and needn't reach their ends.
All inputs are finite; a program needn't handle non-finite values. No bound on the sum of `pair_mask` on one device may be relied on, other than what follows from the above.
Results may differ from the reference program's by a relative error of at most 0.015.
Values may be sent and summed in bfloat16 or wider, within the bound.
No kernel may reach another device: no remote copies, remote signals or barrier semaphores. Data moves between devices by JAX's collectives and lax.ppermute only.
A program may use at most 64 MiB of HBM per device.

```python
import jax
import jax.numpy as jnp
from jax import lax

C = 128
H = 128
N = 512


def place_ends(drawn, own_key, smallest, high):
    spot = [jax.random.randint(jax.random.fold_in(own_key, axis), (), 0, length) for axis, length in enumerate(drawn.shape)]
    widest = drawn.shape.index(max(drawn.shape))
    beside = spot[:widest] + [(spot[widest] + 1) % drawn.shape[widest]] + spot[widest + 1:]
    return drawn.at[tuple(spot)].set(smallest).at[tuple(beside)].set(high)


def shard_levels(own_key, extent, shards, least, high):
    def one(position, parts):
        steps = jax.random.uniform(jax.random.fold_in(jax.random.fold_in(own_key, 6), position), (parts,), jnp.float32, least / len(shards), high / len(shards))
        return jnp.repeat(jnp.exp(steps), extent[position] // parts).reshape((-1,) + (1,) * (len(extent) - position - 1))

    loudness = one(*shards[0])
    for cut in shards[1:]:
        loudness = loudness * one(*cut)
    return loudness


def bell_draw(key, dims, deviation, reach, shards=(), held_as=jnp.bfloat16):
    array = jax.random.normal(key, dims, jnp.float32) * deviation
    if len(shards) > 0:
        array = shard_levels(key, dims, shards, -0.22, 0.18) * array
    return jnp.clip(array, min=-reach, max=reach).astype(held_as)


def setup_inputs(seed: int = 0) -> dict:
    seeds = jax.random.split(jax.random.key(seed), 11)
    pair_repr = bell_draw(seeds[0], (N, N, C), 1.0, 6.0, ((0, 8), (1, 4)))
    pair_mask = place_ends((jax.random.randint(seeds[1], (N, N), 0, 4) < 3).astype(jnp.int32), jax.random.fold_in(seeds[1], 1), 0, 1)
    ln_gain = jnp.clip(1.0 + 0.18 * jax.random.normal(seeds[2], (C,), jnp.float32), 0.1, 1.9)
    ln_bias = bell_draw(seeds[3], (C,), 0.5, 3.0, (), jnp.float32)
    w_proj = bell_draw(seeds[4], (C, 2 * H), C ** -0.5, 0.5)
    w_gate = bell_draw(seeds[5], (C, 2 * H), C ** -0.5, 0.5)
    w_out_gate = bell_draw(seeds[6], (C, C), C ** -0.5, 0.5)
    out_gain = jnp.clip(1.0 + 0.18 * jax.random.normal(seeds[7], (H,), jnp.float32), 0.1, 1.9)
    out_bias = bell_draw(seeds[8], (H,), 0.5, 3.0, (), jnp.float32)
    w_out = bell_draw(seeds[9], (H, C), H ** -0.5, 0.5)
    return dict(pair_repr=pair_repr, pair_mask=pair_mask, ln_gain=ln_gain, ln_bias=ln_bias, w_proj=w_proj, w_gate=w_gate, w_out_gate=w_out_gate, out_gain=out_gain, out_bias=out_bias, w_out=w_out)


def layer_norm(values, gain_vec, bias_vec):
    center = lax.optimization_barrier(jnp.mean(values, axis=-1, keepdims=True))
    deviate = values - center
    spread = lax.optimization_barrier(jnp.mean(deviate * deviate, axis=-1, keepdims=True))
    return deviate * lax.rsqrt(spread + 1e-05) * gain_vec + bias_vec

def reference(pair_repr, pair_mask, ln_gain, ln_bias, w_proj, w_gate, w_out_gate, out_gain, out_bias, w_out):
    normed = layer_norm(pair_repr.astype(jnp.float32), ln_gain, ln_bias).astype(jnp.bfloat16)
    flat_rows = normed.reshape(N * N, C)
    projected = jnp.dot(flat_rows, w_proj, preferred_element_type=jnp.float32)
    gate_logits = jnp.dot(flat_rows, w_gate, preferred_element_type=jnp.float32)
    mask_col = pair_mask.reshape(N * N, 1).astype(jnp.float32)
    edges = (jax.nn.sigmoid(gate_logits) * projected * mask_col).astype(jnp.bfloat16).reshape(N, N, 2 * H)
    left_edge = jnp.transpose(edges[:, :, :H], (2, 0, 1)).astype(jnp.float32)
    right_edge = jnp.transpose(edges[:, :, H:], (2, 1, 0)).astype(jnp.float32)
    triangle = jnp.transpose(jnp.matmul(left_edge, right_edge), (1, 2, 0))
    tri_normed = layer_norm(triangle, out_gain, out_bias).astype(jnp.bfloat16)
    out_gate = jax.nn.sigmoid(jnp.dot(flat_rows, w_out_gate, preferred_element_type=jnp.float32))
    projected_out = jnp.dot(tri_normed.reshape(N * N, H), w_out, preferred_element_type=jnp.float32)
    return (out_gate * projected_out).astype(jnp.bfloat16).reshape(N, N, C)
```

```python
import jax
import jax.numpy as jnp
from jax import lax
from jax.experimental import pallas as pl
from jax.experimental.pallas import tpu as pltpu
from jax.sharding import PartitionSpec as P

EPS = 1e-05
F32 = jnp.float32
BF16 = jnp.bfloat16


def sigmoid(x):
    return 0.5 * jnp.tanh(0.5 * x) + 0.5


def layer_norm(values, gain_vec, bias_vec):
    center = jnp.mean(values, axis=-1, keepdims=True)
    deviate = values - center
    spread = jnp.mean(deviate * deviate, axis=-1, keepdims=True)
    return deviate * lax.rsqrt(spread + EPS) * gain_vec + bias_vec


def contract(a, b, dim_a, dim_b):
    return lax.dot_general(a, b, (((dim_a,), (dim_b,)), ((), ())), preferred_element_type=F32)


def edge_kernel(z_ref, m_ref, gain_ref, bias_ref, wp_ref, wg_ref, out_ref):
    rows, cols, chans = z_ref.shape
    dests, sides, each, _, _ = out_ref.shape
    wp = wp_ref[...]
    wg = wg_ref[...]
    mask = m_ref[...].astype(F32)
    edges = []
    for i in range(rows):
        normed = layer_norm(z_ref[i].astype(F32), gain_ref[...], bias_ref[...]).astype(BF16)
        proj = contract(wp, normed, 0, 1)
        gate = contract(wg, normed, 0, 1)
        edges.append(sigmoid(gate) * proj * mask[i : i + 1, :])
    by_h = jnp.swapaxes(jnp.stack(edges, axis=0), 0, 1).astype(BF16)
    by_h = by_h.reshape(sides, dests, each, rows, cols)
    for s in range(sides):
        out_ref[:, s] = by_h[s]


def gate_kernel(z_ref, gain_ref, bias_ref, w_ref, out_ref):
    rows, cols, chans = z_ref.shape
    flat = z_ref[...].astype(F32).reshape(rows * cols, chans)
    normed = layer_norm(flat, gain_ref[...], bias_ref[...]).astype(BF16)
    gate = sigmoid(contract(normed, w_ref[...], 1, 0))
    out_ref[...] = gate.astype(BF16).reshape(rows, cols, chans)


def make_triangle_kernel(row_parts, col_parts):
    def triangle_kernel(e_ref, out_ref):
        def whole(side):
            return jnp.concatenate(
                [
                    jnp.concatenate(
                        [e_ref[r * col_parts + c, side, 0] for c in range(col_parts)], axis=1
                    )
                    for r in range(row_parts)
                ],
                axis=0,
            )

        tri = contract(whole(0), whole(1), 1, 1).astype(BF16)
        bi = tri.shape[0] // row_parts
        bj = tri.shape[1] // col_parts
        for r in range(row_parts):
            for c in range(col_parts):
                out_ref[r * col_parts + c, 0] = tri[r * bi : (r + 1) * bi, c * bj : (c + 1) * bj]

    return triangle_kernel


def out_kernel(t_ref, g_ref, gain_ref, bias_ref, w_ref, out_ref):
    tri = t_ref[...].astype(F32)
    deviate = tri - jnp.mean(tri, axis=0, keepdims=True)
    spread = jnp.mean(deviate * deviate, axis=0, keepdims=True)
    scaled = jnp.swapaxes(deviate * lax.rsqrt(spread + EPS), 0, 1)
    w = w_ref[...]
    for i in range(scaled.shape[0]):
        normed = (scaled[i] * gain_ref[...] + bias_ref[...]).astype(BF16)
        update = contract(normed, w, 0, 0)
        out_ref[i] = (g_ref[i].astype(F32) * update).astype(BF16)


def whole_spec(array):
    return pl.BlockSpec(array.shape, lambda *_: (0,) * array.ndim)


def make_channel_body(row_parts, col_parts):
    parts = row_parts * col_parts
    axes = ("rows", "ka")

    def body(z, mask, ln_gain, ln_bias, w_proj, w_gate, w_out_gate, out_gain, out_bias, w_out):
        rows, cols, chans = z.shape
        hidden = w_out.shape[0]
        each = hidden // parts
        step = min(16, rows)
        gain_row = ln_gain.reshape(1, chans)
        bias_row = ln_bias.reshape(1, chans)
        par = pltpu.CompilerParams(dimension_semantics=("arbitrary",))
        z_spec = pl.BlockSpec((step, cols, chans), lambda i: (i, 0, 0))
        edges = pl.pallas_call(
            edge_kernel,
            grid=(rows // step,),
            in_specs=[
                z_spec,
                pl.BlockSpec((step, cols), lambda i: (i, 0)),
                whole_spec(gain_row),
                whole_spec(bias_row),
                whole_spec(w_proj),
                whole_spec(w_gate),
            ],
            out_specs=pl.BlockSpec((parts, 2, each, step, cols), lambda i: (0, 0, 0, i, 0)),
            out_shape=jax.ShapeDtypeStruct((parts, 2, each, rows, cols), BF16),
            compiler_params=par,
            name="edges",
        )(z, mask, gain_row, bias_row, w_proj, w_gate)
        mine = lax.all_to_all(edges, axes, 0, 0, tiled=True)
        out_gate = pl.pallas_call(
            gate_kernel,
            grid=(rows // step,),
            in_specs=[z_spec, whole_spec(gain_row), whole_spec(bias_row), whole_spec(w_out_gate)],
            out_specs=z_spec,
            out_shape=jax.ShapeDtypeStruct((rows, cols, chans), BF16),
            compiler_params=par,
            name="out_gate",
        )(z, gain_row, bias_row, w_out_gate)
        sums = pl.pallas_call(
            make_triangle_kernel(row_parts, col_parts),
            grid=(each,),
            in_specs=[pl.BlockSpec((parts, 2, 1, rows, cols), lambda h: (0, 0, h, 0, 0))],
            out_specs=pl.BlockSpec((parts, 1, rows, cols), lambda h: (0, h, 0, 0)),
            out_shape=jax.ShapeDtypeStruct((parts, each, rows, cols), BF16),
            compiler_params=par,
            name="triangle",
        )(mine)
        tri = lax.all_to_all(sums, axes, 0, 0, tiled=True).reshape(hidden, rows, cols)
        gain_wide = jnp.broadcast_to(out_gain.reshape(hidden, 1), (hidden, cols))
        bias_wide = jnp.broadcast_to(out_bias.reshape(hidden, 1), (hidden, cols))
        return pl.pallas_call(
            out_kernel,
            grid=(rows // step,),
            in_specs=[
                pl.BlockSpec((hidden, step, cols), lambda i: (0, i, 0)),
                z_spec,
                whole_spec(gain_wide),
                whole_spec(bias_wide),
                whole_spec(w_out),
            ],
            out_specs=z_spec,
            out_shape=jax.ShapeDtypeStruct((rows, cols, chans), BF16),
            compiler_params=par,
            name="update",
        )(tri, out_gate, gain_wide, bias_wide, w_out)

    return body


def gathered_body(z, mask, ln_gain, ln_bias, w_proj, w_gate, w_out_gate, out_gain, out_bias, w_out):
    rows, cols, chans = z.shape
    hidden = w_out.shape[0]
    normed = layer_norm(z.astype(F32), ln_gain, ln_bias).astype(BF16)
    flat = normed.reshape(rows * cols, chans)
    projected = jnp.dot(flat, w_proj, preferred_element_type=F32)
    gate_logits = jnp.dot(flat, w_gate, preferred_element_type=F32)
    mask_col = mask.reshape(rows * cols, 1).astype(F32)
    edges = (jax.nn.sigmoid(gate_logits) * projected * mask_col).astype(BF16)
    edges = edges.reshape(rows, cols, 2 * hidden)
    partial_sums = jnp.einsum(
        "ikh,jkh->ijh",
        edges[:, :, :hidden],
        lax.all_gather(edges[:, :, hidden:], "rows", axis=0, tiled=True),
        preferred_element_type=F32,
    )
    triangle = lax.psum_scatter(
        partial_sums.astype(BF16), "ka", scatter_dimension=1, tiled=True
    ).astype(F32)
    tri_normed = layer_norm(triangle, out_gain, out_bias).astype(BF16)
    out_gate = jax.nn.sigmoid(jnp.dot(flat, w_out_gate, preferred_element_type=F32))
    projected_out = jnp.dot(
        tri_normed.reshape(rows * cols, hidden), w_out, preferred_element_type=F32
    )
    return (out_gate * projected_out).astype(BF16).reshape(rows, cols, chans)


def solution(mesh):
    row_parts, col_parts = mesh.shape["rows"], mesh.shape["ka"]
    channel_body = make_channel_body(row_parts, col_parts)

    def body(*args):
        hidden = args[-1].shape[0]
        if hidden % (row_parts * col_parts) == 0:
            return channel_body(*args)
        return gathered_body(*args)

    placed = (P("rows", "ka", None), P("rows", "ka"), P(), P(), P(), P(), P(), P(), P(), P())
    return jax.shard_map(
        body, mesh=mesh, in_specs=placed, out_specs=P("rows", "ka", None), check_vma=False
    )
```

```python
import jax
import jax.numpy as jnp
from jax import lax
from jax.experimental import pallas as pl
from jax.experimental.pallas import tpu as pltpu
from jax.sharding import PartitionSpec as P

EPS = 1e-05
F32 = jnp.float32
BF16 = jnp.bfloat16


def sigmoid(x):
    return 0.5 * jnp.tanh(0.5 * x) + 0.5


def layer_norm(values, gain_vec, bias_vec):
    center = jnp.mean(values, axis=-1, keepdims=True)
    deviate = values - center
    spread = jnp.mean(deviate * deviate, axis=-1, keepdims=True)
    return deviate * lax.rsqrt(spread + EPS) * gain_vec + bias_vec


def contract(a, b, dim_a, dim_b):
    return lax.dot_general(a, b, (((dim_a,), (dim_b,)), ((), ())), preferred_element_type=F32)


def row_norm(z, gain_row, bias_row):
    chans = z.shape[-1]
    ones = jnp.ones((chans, chans), BF16)
    deviate = z.astype(F32) - contract(z, ones, 1, 0) * (1.0 / chans)
    square = deviate * deviate
    high = square.astype(BF16)
    low = (square - high.astype(F32)).astype(BF16)
    spread = (contract(high, ones, 1, 0) + contract(low, ones, 1, 0)) * (1.0 / chans)
    return (deviate * lax.rsqrt(spread + EPS) * gain_row + bias_row).astype(BF16)


def edge_kernel(z_ref, m_ref, gain_ref, bias_ref, wp_ref, wg_ref, out_ref):
    rows, cols, chans = z_ref.shape
    dests, sides, each, _, _ = out_ref.shape
    both = jnp.concatenate([wp_ref[...].T, wg_ref[...].T], axis=0)
    mask = m_ref[...].astype(F32)
    flat = row_norm(z_ref[...].reshape(rows * cols, chans), gain_ref[...], bias_ref[...])
    width = sides * dests * each
    edges = []
    for i in range(rows):
        made = contract(both, flat[i * cols : (i + 1) * cols], 1, 1)
        edges.append(sigmoid(made[width:]) * made[:width] * mask[i : i + 1, :])
    by_h = jnp.swapaxes(jnp.stack(edges, axis=0), 0, 1).astype(BF16)
    by_h = by_h.reshape(sides, dests, each, rows, cols)
    for s in range(sides):
        out_ref[:, s] = by_h[s]


def gate_kernel(z_ref, gain_ref, bias_ref, w_ref, out_ref):
    rows, cols, chans = z_ref.shape
    flat = row_norm(z_ref[...].reshape(rows * cols, chans), gain_ref[...], bias_ref[...])
    gate = sigmoid(contract(flat, w_ref[...], 1, 0))
    out_ref[...] = gate.astype(BF16).reshape(rows, cols, chans)


def make_triangle_kernel(row_parts, col_parts):
    def triangle_kernel(e_ref, out_ref):
        def whole(side):
            return jnp.concatenate(
                [
                    jnp.concatenate(
                        [e_ref[r * col_parts + c, side, 0] for c in range(col_parts)], axis=1
                    )
                    for r in range(row_parts)
                ],
                axis=0,
            )

        tri = contract(whole(0), whole(1), 1, 1).astype(BF16)
        bi = tri.shape[0] // row_parts
        bj = tri.shape[1] // col_parts
        for r in range(row_parts):
            for c in range(col_parts):
                out_ref[r * col_parts + c, 0] = tri[r * bi : (r + 1) * bi, c * bj : (c + 1) * bj]

    return triangle_kernel


def out_kernel(t_ref, g_ref, gain_ref, bias_ref, w_ref, out_ref):
    tri = t_ref[...].astype(F32)
    deviate = tri - jnp.mean(tri, axis=0, keepdims=True)
    spread = jnp.mean(deviate * deviate, axis=0, keepdims=True)
    scaled = jnp.swapaxes(deviate * lax.rsqrt(spread + EPS), 0, 1)
    w = w_ref[...]
    hidden, cols = scaled.shape[1:]
    gain = jnp.broadcast_to(gain_ref[...], (cols, hidden)).T
    bias = jnp.broadcast_to(bias_ref[...], (cols, hidden)).T
    for i in range(scaled.shape[0]):
        normed = (scaled[i] * gain + bias).astype(BF16)
        update = contract(normed, w, 0, 0)
        out_ref[i] = (g_ref[i].astype(F32) * update).astype(BF16)


def whole_spec(array):
    return pl.BlockSpec(array.shape, lambda *_: (0,) * array.ndim)


def make_channel_body(row_parts, col_parts):
    parts = row_parts * col_parts
    axes = ("rows", "ka")

    def body(z, mask, ln_gain, ln_bias, w_proj, w_gate, w_out_gate, out_gain, out_bias, w_out):
        rows, cols, chans = z.shape
        hidden = w_out.shape[0]
        each = hidden // parts
        step = min(32, rows)
        gain_row = ln_gain.reshape(1, chans)
        bias_row = ln_bias.reshape(1, chans)
        par = pltpu.CompilerParams(dimension_semantics=("arbitrary",))
        z_spec = pl.BlockSpec((step, cols, chans), lambda i: (i, 0, 0))
        edges = pl.pallas_call(
            edge_kernel,
            grid=(rows // step,),
            in_specs=[
                z_spec,
                pl.BlockSpec((step, cols), lambda i: (i, 0)),
                whole_spec(gain_row),
                whole_spec(bias_row),
                whole_spec(w_proj),
                whole_spec(w_gate),
            ],
            out_specs=pl.BlockSpec((parts, 2, each, step, cols), lambda i: (0, 0, 0, i, 0)),
            out_shape=jax.ShapeDtypeStruct((parts, 2, each, rows, cols), BF16),
            compiler_params=par,
            name="edges",
        )(z, mask, gain_row, bias_row, w_proj, w_gate)
        mine = lax.all_to_all(edges, axes, 0, 0, tiled=True)
        out_gate = pl.pallas_call(
            gate_kernel,
            grid=(rows // step,),
            in_specs=[z_spec, whole_spec(gain_row), whole_spec(bias_row), whole_spec(w_out_gate)],
            out_specs=z_spec,
            out_shape=jax.ShapeDtypeStruct((rows, cols, chans), BF16),
            compiler_params=par,
            name="out_gate",
        )(z, gain_row, bias_row, w_out_gate)
        sums = pl.pallas_call(
            make_triangle_kernel(row_parts, col_parts),
            grid=(each,),
            in_specs=[pl.BlockSpec((parts, 2, 1, rows, cols), lambda h: (0, 0, h, 0, 0))],
            out_specs=pl.BlockSpec((parts, 1, rows, cols), lambda h: (0, h, 0, 0)),
            out_shape=jax.ShapeDtypeStruct((parts, each, rows, cols), BF16),
            compiler_params=par,
            name="triangle",
        )(mine)
        tri = lax.all_to_all(sums, axes, 0, 0, tiled=True).reshape(hidden, rows, cols)
        gain_out = out_gain.reshape(1, hidden)
        bias_out = out_bias.reshape(1, hidden)
        return pl.pallas_call(
            out_kernel,
            grid=(rows // step,),
            in_specs=[
                pl.BlockSpec((hidden, step, cols), lambda i: (0, i, 0)),
                z_spec,
                whole_spec(gain_out),
                whole_spec(bias_out),
                whole_spec(w_out),
            ],
            out_specs=z_spec,
            out_shape=jax.ShapeDtypeStruct((rows, cols, chans), BF16),
            compiler_params=par,
            name="update",
        )(tri, out_gate, gain_out, bias_out, w_out)

    return body


def gathered_body(z, mask, ln_gain, ln_bias, w_proj, w_gate, w_out_gate, out_gain, out_bias, w_out):
    rows, cols, chans = z.shape
    hidden = w_out.shape[0]
    normed = layer_norm(z.astype(F32), ln_gain, ln_bias).astype(BF16)
    flat = normed.reshape(rows * cols, chans)
    projected = jnp.dot(flat, w_proj, preferred_element_type=F32)
    gate_logits = jnp.dot(flat, w_gate, preferred_element_type=F32)
    mask_col = mask.reshape(rows * cols, 1).astype(F32)
    edges = (jax.nn.sigmoid(gate_logits) * projected * mask_col).astype(BF16)
    edges = edges.reshape(rows, cols, 2 * hidden)
    partial_sums = jnp.einsum(
        "ikh,jkh->ijh",
        edges[:, :, :hidden],
        lax.all_gather(edges[:, :, hidden:], "rows", axis=0, tiled=True),
        preferred_element_type=F32,
    )
    triangle = lax.psum_scatter(
        partial_sums.astype(BF16), "ka", scatter_dimension=1, tiled=True
    ).astype(F32)
    tri_normed = layer_norm(triangle, out_gain, out_bias).astype(BF16)
    out_gate = jax.nn.sigmoid(jnp.dot(flat, w_out_gate, preferred_element_type=F32))
    projected_out = jnp.dot(
        tri_normed.reshape(rows * cols, hidden), w_out, preferred_element_type=F32
    )
    return (out_gate * projected_out).astype(BF16).reshape(rows, cols, chans)


def solution(mesh):
    row_parts, col_parts = mesh.shape["rows"], mesh.shape["ka"]
    channel_body = make_channel_body(row_parts, col_parts)

    def body(*args):
        hidden = args[-1].shape[0]
        if hidden % (row_parts * col_parts) == 0:
            return channel_body(*args)
        return gathered_body(*args)

    placed = (P("rows", "ka", None), P("rows", "ka"), P(), P(), P(), P(), P(), P(), P(), P())
    return jax.shard_map(
        body, mesh=mesh, in_specs=placed, out_specs=P("rows", "ka", None), check_vma=False
    )
```
